8 devices in a mesh: dp: 2 (over z, y), fsdp: 4 (over x, core).
Axes of the slice: x: 2, y: 2, z: 1, core: 2. Of those that a mesh axis runs over, the one named last changes fastest.
Arguments:
- tokens: bfloat16 [512, 77, 1024], P(('dp', 'fsdp'))
- grad_out: bfloat16 [512, 77, 1024], P(('dp', 'fsdp'))
- ln1_gain: float32 [2, 1024], P(None, 'fsdp')
- ln1_shift: float32 [2, 1024], P(None, 'fsdp')
- qkv_weight: float32 [2, 1024, 3072], P(None, 'fsdp')
- qkv_bias: float32 [2, 3072], P(None, 'fsdp')
- out_weight: float32 [2, 1024, 1024], P(None, 'fsdp')
- out_bias: float32 [2, 1024], P(None, 'fsdp')
- ln2_gain: float32 [2, 1024], P(None, 'fsdp')
- ln2_shift: float32 [2, 1024], P(None, 'fsdp')
- fc_weight: float32 [2, 1024, 4096], P(None, 'fsdp')
- fc_bias: float32 [2, 4096], P(None, 'fsdp')
- proj_weight: float32 [2, 4096, 1024], P(None, 'fsdp')
- proj_bias: float32 [2, 1024], P(None, 'fsdp')
Outputs:
- output 1: bfloat16 [512, 77, 1024], P(('dp', 'fsdp'))
- output 2: float32 [2, 1024], P(None, 'fsdp')
- output 3: float32 [2, 1024], P(None, 'fsdp')
- output 4: float32 [2, 1024, 3072], P(None, 'fsdp')
- output 5: float32 [2, 3072], P(None, 'fsdp')
- output 6: float32 [2, 1024, 1024], P(None, 'fsdp')
- output 7: float32 [2, 1024], P(None, 'fsdp')
- output 8: float32 [2, 1024], P(None, 'fsdp')
- output 9: float32 [2, 1024], P(None, 'fsdp')
- output 10: float32 [2, 1024, 4096], P(None, 'fsdp')
- output 11: float32 [2, 4096], P(None, 'fsdp')
- output 12: float32 [2, 4096, 1024], P(None, 'fsdp')
- output 13: float32 [2, 1024], P(None, 'fsdp')
All inputs are finite; a program needn't handle non-finite values.
Results may differ from the reference program's by a relative error of at most 0.0168481.
Values are sent between devices in bfloat16 or wider.
A program may use at most 1 GiB of HBM per device.

```python
import jax
import jax.numpy as jnp
from jax import lax

CAPTIONS = 512
CONTEXT = 77
MODEL_WIDTH = 1024
NUM_HEADS = 16
MLP_WIDTH = 4096
HEAD_DIM = 64
SPLIT = max(1, CAPTIONS // 16)
GROUP = CAPTIONS // SPLIT
SCALE = HEAD_DIM ** -0.5
NORM_EPS = 1e-5


def setup_inputs(seed: int = 0) -> dict:
    keys = jax.random.split(jax.random.key(seed), 14)
    tok_shape = (CAPTIONS, CONTEXT, MODEL_WIDTH)

    def normal(index, shape):
        return jax.random.normal(keys[index], shape, jnp.float32)

    return {
        'tokens': normal(0, tok_shape).astype(jnp.bfloat16),
        'grad_out': (normal(1, tok_shape) * (CAPTIONS * CONTEXT) ** -0.5).astype(jnp.bfloat16),
        'ln1_gain': 1.0 + 0.2 * normal(2, (2, MODEL_WIDTH)),
        'ln1_shift': 0.2 * normal(3, (2, MODEL_WIDTH)),
        'qkv_weight': normal(4, (2, MODEL_WIDTH, 3 * MODEL_WIDTH)) * MODEL_WIDTH ** -0.5,
        'qkv_bias': 0.2 * normal(5, (2, 3 * MODEL_WIDTH)),
        'out_weight': normal(6, (2, MODEL_WIDTH, MODEL_WIDTH)) * MODEL_WIDTH ** -0.5,
        'out_bias': 0.2 * normal(7, (2, MODEL_WIDTH)),
        'ln2_gain': 1.0 + 0.2 * normal(8, (2, MODEL_WIDTH)),
        'ln2_shift': 0.2 * normal(9, (2, MODEL_WIDTH)),
        'fc_weight': normal(10, (2, MODEL_WIDTH, MLP_WIDTH)) * MODEL_WIDTH ** -0.5,
        'fc_bias': 0.2 * normal(11, (2, MLP_WIDTH)),
        'proj_weight': normal(12, (2, MLP_WIDTH, MODEL_WIDTH)) * MLP_WIDTH ** -0.5,
        'proj_bias': 0.2 * normal(13, (2, MODEL_WIDTH)),
    }


def as_bf16(value):
    return value.astype(jnp.bfloat16).astype(jnp.float32)


def layer_norm(hidden, gain, shift):
    centered = hidden - jnp.mean(hidden, axis=-1, keepdims=True)
    variance = jnp.mean(centered * centered, axis=-1, keepdims=True)
    return as_bf16(centered * lax.rsqrt(variance + NORM_EPS) * gain + shift)


def block(hidden, layer):
    ln1_gain, ln1_shift, qkv_weight, qkv_bias, out_weight, out_bias, ln2_gain, ln2_shift, fc_weight, fc_bias, proj_weight, proj_bias = layer
    captions = hidden.shape[0]
    normed1 = layer_norm(hidden, ln1_gain, ln1_shift)
    qkv = as_bf16(jnp.einsum('btw,wc->btc', normed1, qkv_weight) + qkv_bias)
    grouped = qkv.reshape(captions, CONTEXT, 3, NUM_HEADS, HEAD_DIM)
    scores = jnp.einsum('bqhd,bkhd->bhqk', grouped[:, :, 0], grouped[:, :, 1]) * SCALE
    causal = jnp.arange(CONTEXT)[:, None] >= jnp.arange(CONTEXT)[None, :]
    probs = as_bf16(jax.nn.softmax(jnp.where(causal, scores, -1e30), axis=-1))
    context = as_bf16(jnp.einsum('bhqk,bkhd->bqhd', probs, grouped[:, :, 2]))
    context = context.reshape(captions, CONTEXT, MODEL_WIDTH)
    middle = as_bf16(hidden + jnp.einsum('btw,wv->btv', context, out_weight) + out_bias)
    normed2 = layer_norm(middle, ln2_gain, ln2_shift)
    pre_act = jnp.einsum('btw,wf->btf', normed2, fc_weight) + fc_bias
    hidden_mlp = as_bf16(jax.nn.gelu(pre_act, approximate=False))
    return as_bf16(middle + jnp.einsum('btf,fw->btw', hidden_mlp, proj_weight) + proj_bias)


def two_blocks(layers, tokens):
    first = tuple(param[0] for param in layers)
    second = tuple(param[1] for param in layers)
    return block(block(tokens, first), second)


def reference(tokens, grad_out, ln1_gain, ln1_shift, qkv_weight, qkv_bias, out_weight, out_bias, ln2_gain, ln2_shift, fc_weight, fc_bias, proj_weight, proj_bias):
    stored = (ln1_gain, ln1_shift, qkv_weight, qkv_bias, out_weight, out_bias, ln2_gain, ln2_shift, fc_weight, fc_bias, proj_weight, proj_bias)
    layers = tuple(param.astype(jnp.bfloat16).astype(jnp.float32) for param in stored)
    tok_groups = tokens.astype(jnp.float32).reshape(SPLIT, GROUP, CONTEXT, MODEL_WIDTH)
    grad_groups = grad_out.astype(jnp.float32).reshape(SPLIT, GROUP, CONTEXT, MODEL_WIDTH)

    def group_step(totals, pair):
        tok_group, grad_group = pair

        def forward(params):
            return two_blocks(params, tok_group)

        out_group, pullback = jax.vjp(forward, layers)
        grads = pullback(grad_group)[0]
        new_totals = tuple(total + grad for total, grad in zip(totals, grads))
        return new_totals, out_group.astype(jnp.bfloat16)

    start = tuple(jnp.zeros_like(param) for param in layers)
    sums, outs = lax.scan(group_step, start, (tok_groups, grad_groups))
    block_out = outs.reshape(CAPTIONS, CONTEXT, MODEL_WIDTH)
    return (block_out, sums[0], sums[1], sums[2], sums[3], sums[4], sums[5], sums[6], sums[7], sums[8], sums[9], sums[10], sums[11])
```

```python
import functools
import math

import jax
import jax.numpy as jnp
from jax import lax
from jax.experimental import pallas as pl
from jax.experimental.pallas import tpu as pltpu
from jax.sharding import PartitionSpec as P

HEAD_DIM = 64
NORM_EPS = 1e-5
RANKS = (2, 2, 3, 2, 3, 2, 2, 2, 3, 2, 3, 2)
BIG = (2, 4, 8, 10)
SMALL = (0, 1, 3, 5, 6, 7, 9, 11)
F32 = jnp.float32
BF16 = jnp.bfloat16
NT = (((1,), (1,)), ((), ()))
NN = (((1,), (0,)), ((), ()))
TN = (((0,), (0,)), ((), ()))
EXP_SCALE = math.log2(math.e) / 8.0


def mm(lhs, rhs, dims):
    return lax.dot_general(lhs, rhs, dims, preferred_element_type=F32)


def pair_masks(length):
    lane = lax.broadcasted_iota(jnp.int32, (length, 128), 1) < HEAD_DIM
    query = lax.broadcasted_iota(jnp.int32, (length, 256), 1) & 127
    key = lax.broadcasted_iota(jnp.int32, (length, 256), 0)
    return lane, key <= query


def attn_fwd_kernel(qkv_ref, out_ref, q_blocks, score_buf):
    captions, length, width = out_ref.shape

    @pl.when(pl.program_id(0) == 0)
    def _():
        q_blocks[...] = jnp.zeros_like(q_blocks)

    lane, causal = pair_masks(length)
    zero = jnp.zeros((length, 128), BF16)

    def caption(index, carry):
        for pair in range(width // 128):
            query = qkv_ref[index, :, 128 * pair:128 * pair + 128]
            q_blocks[pair, 0:length] = jnp.where(lane, query, zero)
            q_blocks[pair, 128:128 + length] = jnp.where(lane, zero, query)
        for pair in range(width // 128):
            keys = qkv_ref[index, :, width + 128 * pair:width + 128 * pair + 128]
            score_buf[pair] = mm(keys, q_blocks[pair], NT)
        for pair in range(width // 128):
            values = qkv_ref[index, :, 2 * width + 128 * pair:2 * width + 128 * pair + 128]
            scores = jnp.where(causal, score_buf[pair], -1e30)
            weights = jnp.exp2((scores - jnp.max(scores, axis=0, keepdims=True)) * EXP_SCALE)
            probs = (weights * (1.0 / jnp.sum(weights, axis=0, keepdims=True))).astype(BF16)
            both = mm(probs, values, TN)
            out_ref[index, :, 128 * pair:128 * pair + 128] = jnp.where(lane, both[0:length], both[128:128 + length]).astype(BF16)
        return carry

    lax.fori_loop(0, captions, caption, 0)


def attn_bwd_kernel(qkv_ref, d_out_ref, d_qkv_ref, q_blocks, d_blocks, score_buf, d_prob_buf):
    captions, length, width = d_out_ref.shape

    @pl.when(pl.program_id(0) == 0)
    def _():
        q_blocks[...] = jnp.zeros_like(q_blocks)
        d_blocks[...] = jnp.zeros_like(d_blocks)

    lane, causal = pair_masks(length)
    zero = jnp.zeros((length, 128), BF16)

    def caption(index, carry):
        for pair in range(width // 128):
            at = 128 * pair
            query = qkv_ref[index, :, at:at + 128]
            d_out = d_out_ref[index, :, at:at + 128]
            q_blocks[pair, 0:length] = jnp.where(lane, query, zero)
            q_blocks[pair, 128:128 + length] = jnp.where(lane, zero, query)
            d_blocks[pair, 0:length] = jnp.where(lane, d_out, zero)
            d_blocks[pair, 128:128 + length] = jnp.where(lane, zero, d_out)
        for pair in range(width // 128):
            at = 128 * pair
            score_buf[pair] = mm(qkv_ref[index, :, width + at:width + at + 128], q_blocks[pair], NT)
            d_prob_buf[pair] = mm(qkv_ref[index, :, 2 * width + at:2 * width + at + 128], d_blocks[pair], NT)
        for pair in range(width // 128):
            at = 128 * pair
            keys = qkv_ref[index, :, width + at:width + at + 128]
            scores = jnp.where(causal, score_buf[pair], -1e30)
            d_probs = d_prob_buf[pair].astype(BF16).astype(F32)
            weights = jnp.exp2((scores - jnp.max(scores, axis=0, keepdims=True)) * EXP_SCALE)
            probs = weights * (1.0 / jnp.sum(weights, axis=0, keepdims=True))
            inner = jnp.sum(probs * d_probs, axis=0, keepdims=True)
            d_scores = (probs * ((d_probs - inner) * (HEAD_DIM ** -0.5))).astype(BF16)
            d_query = mm(d_scores, keys, TN)
            d_qkv_ref[index, :, at:at + 128] = jnp.where(lane, d_query[0:length], d_query[128:128 + length]).astype(BF16)
            d_qkv_ref[index, :, width + at:width + at + 128] = mm(d_scores, q_blocks[pair], NN).astype(BF16)
            d_qkv_ref[index, :, 2 * width + at:2 * width + at + 128] = mm(probs.astype(BF16), d_blocks[pair], NN).astype(BF16)
        return carry

    lax.fori_loop(0, captions, caption, 0)


def attn_call(kernel, name, out_width, operands, flops):
    captions, length, _ = operands[0].shape
    width = operands[0].shape[2] // 3
    step = 4
    blocks = pltpu.VMEM((width // 128, 256, 128), BF16)
    scores = pltpu.VMEM((width // 128, length, 256), F32)
    copies = len(operands)
    return pl.pallas_call(
        kernel,
        grid=(captions // step,),
        in_specs=[pl.BlockSpec((step, length, x.shape[2]), lambda i: (i, 0, 0)) for x in operands],
        out_specs=pl.BlockSpec((step, length, out_width), lambda i: (i, 0, 0)),
        out_shape=jax.ShapeDtypeStruct((captions, length, out_width), BF16),
        scratch_shapes=[blocks] * copies + [scores] * copies,
        compiler_params=pltpu.CompilerParams(dimension_semantics=("arbitrary",), vmem_limit_bytes=48 * 2**20),
        cost_estimate=pl.CostEstimate(flops=flops, transcendentals=0, bytes_accessed=sum(2 * x.size for x in operands)),
        name=name,
    )(*operands)


def attn_fwd(qkv, length):
    rows, wide = qkv.shape
    by_caption = qkv.reshape(length, rows // length, wide).transpose(1, 0, 2)
    context = attn_call(attn_fwd_kernel, "attn_fwd", wide // 3, (by_caption,), 40 * 10**9)
    return context.transpose(1, 0, 2).reshape(rows, wide // 3), by_caption


def attn_bwd(d_context, by_caption, length):
    rows, width = d_context.shape
    d_by_caption = d_context.reshape(length, rows // length, width).transpose(1, 0, 2)
    d_qkv = attn_call(attn_bwd_kernel, "attn_bwd", 3 * width, (by_caption, d_by_caption), 60 * 10**9)
    return d_qkv.transpose(1, 0, 2).reshape(rows, 3 * width)


def norm_stats(source):
    src32 = source.astype(F32)
    centered = src32 - jnp.mean(src32, axis=-1, keepdims=True)
    inv_std = lax.rsqrt(jnp.mean(centered * centered, axis=-1, keepdims=True) + NORM_EPS)
    return centered * inv_std, inv_std


def norm_fwd(source, gain, shift):
    normed, _ = norm_stats(source)
    return (normed * gain + shift).astype(BF16)


def norm_bwd(d_out, source, gain, want_input):
    normed, inv_std = norm_stats(source)
    d_gain = jnp.sum(d_out * normed, axis=0)
    d_shift = jnp.sum(d_out, axis=0)
    if not want_input:
        return None, d_gain, d_shift
    d_norm = d_out * gain
    d_source = inv_std * (d_norm - jnp.mean(d_norm, axis=-1, keepdims=True) - normed * jnp.mean(d_norm * normed, axis=-1, keepdims=True))
    return d_source, d_gain, d_shift


def gelu_cdf(pre_act):
    return 0.5 * (1.0 + lax.erf(pre_act * 0.7071067811865476))


def gelu_grad(pre_act):
    return gelu_cdf(pre_act) + pre_act * jnp.exp(-0.5 * pre_act * pre_act) * 0.3989422804014327


def block_fwd(tokens, big, small, length):
    qkv_weight, out_weight, fc_weight, proj_weight = big
    ln1_gain, ln1_shift, qkv_bias, out_bias, ln2_gain, ln2_shift, fc_bias, proj_bias = small
    normed1 = norm_fwd(tokens, ln1_gain, ln1_shift)
    qkv = (mm(normed1, qkv_weight, NN) + qkv_bias).astype(BF16)
    context, by_caption = attn_fwd(qkv, length)
    middle = (tokens.astype(F32) + mm(context, out_weight, NN) + out_bias).astype(BF16)
    normed2 = norm_fwd(middle, ln2_gain, ln2_shift)
    pre_act = mm(normed2, fc_weight, NN) + fc_bias
    hidden = (pre_act * gelu_cdf(pre_act)).astype(BF16)
    result = (middle.astype(F32) + mm(hidden, proj_weight, NN) + proj_bias).astype(BF16)
    return result, (tokens, normed1, by_caption, context, middle, normed2, pre_act, hidden)


def block_bwd(d_result, saved, big, small, length, want_input, reduce_grad):
    qkv_weight, out_weight, fc_weight, proj_weight = big
    ln1_gain, _, _, _, ln2_gain, _, _, _ = small
    tokens, normed1, by_caption, context, middle, normed2, pre_act, hidden = saved
    d_res32 = d_result.astype(F32)
    g_proj_bias = jnp.sum(d_res32, axis=0)
    g_proj_weight = mm(hidden, d_result, TN)
    d_result, g_proj_weight = lax.optimization_barrier((d_result, g_proj_weight))
    r_proj = reduce_grad(g_proj_weight)
    d_hidden = mm(d_result, proj_weight, NT).astype(BF16).astype(F32)
    d_pre = d_hidden * gelu_grad(pre_act)
    g_fc_bias = jnp.sum(d_pre, axis=0)
    d_pre = d_pre.astype(BF16)
    g_fc_weight = mm(normed2, d_pre, TN)
    d_pre, g_fc_weight = lax.optimization_barrier((d_pre, g_fc_weight))
    r_fc = reduce_grad(g_fc_weight)
    d_normed2 = mm(d_pre, fc_weight, NT).astype(BF16).astype(F32)
    d_mid_norm, g_ln2_gain, g_ln2_shift = norm_bwd(d_normed2, middle, ln2_gain, True)
    d_middle = (d_res32 + d_mid_norm).astype(BF16)
    g_out_bias = jnp.sum(d_middle, axis=0, dtype=F32)
    g_out_weight = mm(context, d_middle, TN)
    d_middle, g_out_weight = lax.optimization_barrier((d_middle, g_out_weight))
    r_out = reduce_grad(g_out_weight)
    d_context = mm(d_middle, out_weight, NT).astype(BF16)
    d_qkv = attn_bwd(d_context, by_caption, length)
    g_qkv_bias = jnp.sum(d_qkv, axis=0, dtype=F32)
    g_qkv_weight = mm(normed1, d_qkv, TN)
    d_qkv, g_qkv_weight = lax.optimization_barrier((d_qkv, g_qkv_weight))
    r_qkv = reduce_grad(g_qkv_weight)
    d_normed1 = mm(d_qkv, qkv_weight, NT).astype(BF16).astype(F32)
    d_tok_norm, g_ln1_gain, g_ln1_shift = norm_bwd(d_normed1, tokens, ln1_gain, want_input)
    d_tokens = None
    if want_input:
        d_tokens = (d_middle.astype(F32) + d_tok_norm).astype(BF16)
    small_grads = (g_ln1_gain, g_ln1_shift, g_qkv_bias, g_out_bias, g_ln2_gain, g_ln2_shift, g_fc_bias, g_proj_bias)
    return d_tokens, (r_qkv, r_out, r_fc, r_proj), small_grads


def solution(mesh):
    batch_spec = P(('dp', 'fsdp'), None, None)
    param_specs = tuple(P(None, 'fsdp', None) if rank == 3 else P(None, 'fsdp') for rank in RANKS)
    shards = mesh.shape['fsdp']
    copies = mesh.shape['dp']
    swap = [(i, (i + 1) % copies) for i in range(copies)]

    def reduce_grad(grad):
        own = lax.psum_scatter(grad, 'fsdp', scatter_dimension=0, tiled=True)
        return own, lax.ppermute(own, 'dp', swap)

    def per_device(tokens, grad_out, *params):
        captions, length, width = tokens.shape
        rows = captions * length
        small_sizes = [params[i].shape[1] for i in SMALL]
        small_all = lax.all_gather(jnp.concatenate([params[i].astype(BF16) for i in SMALL], axis=1), 'fsdp', axis=0, tiled=False)

        def small_of(layer):
            found, at = [], 0
            for size in small_sizes:
                found.append(small_all[:, layer, at:at + size].reshape(-1).astype(F32))
                at += size
            return tuple(found)

        def big_of(layer):
            return tuple(lax.all_gather(params[i][layer].astype(BF16), 'fsdp', axis=0, tiled=True) for i in BIG)

        big0, big1 = big_of(0), big_of(1)
        small0, small1 = small_of(0), small_of(1)
        flat = tokens.transpose(1, 0, 2).reshape(rows, width)
        d_flat = grad_out.transpose(1, 0, 2).reshape(rows, width)
        mid_tokens, saved0 = block_fwd(flat, big0, small0, length)
        block_out, saved1 = block_fwd(mid_tokens, big1, small1, length)
        d_mid, wide1, narrow1 = block_bwd(d_flat, saved1, big1, small1, length, True, reduce_grad)
        _, wide0, narrow0 = block_bwd(d_mid, saved0, big0, small0, length, False, reduce_grad)

        split = [[grad.reshape(shards, 1, -1) for grad in narrow] for narrow in (narrow0, narrow1)]
        packed = jnp.concatenate([jnp.concatenate(row, axis=2) for row in split], axis=1)
        summed = lax.psum(packed, ('dp', 'fsdp'))
        mine = lax.dynamic_index_in_dim(summed, lax.axis_index('fsdp'), 0, keepdims=False)
        grads = [None] * len(RANKS)
        at = 0
        for i, size in zip(SMALL, small_sizes):
            grads[i] = mine[:, at:at + size]
            at += size
        for i, first, second in zip(BIG, wide0, wide1):
            grads[i] = jnp.stack([first[0] + first[1], second[0] + second[1]])
        block_out = block_out.reshape(length, captions, width).transpose(1, 0, 2)
        return (block_out,) + tuple(grads)

    return jax.shard_map(per_device, mesh=mesh, in_specs=(batch_spec, batch_spec) + param_specs, out_specs=(batch_spec,) + param_specs, check_vma=False)
```
